32 devices in a mesh: cfg: 2 (over x), seq: 8 (over z, y), dp: 2 (over core).
Axes of the slice: x: 2, y: 2, z: 4, core: 2. Of those that a mesh axis runs over, the one named last changes fastest.
Arguments:
- teacher_query: bfloat16 [2, 2, 2, 1024, 2048], P('cfg', None, 'dp', 'seq'), may hold values from -6 to 6
- teacher_key: bfloat16 [2, 2, 2, 1024, 2048], P('cfg', None, 'dp', 'seq'), may hold values from -6 to 6
- teacher_value: bfloat16 [2, 2, 2, 1024, 2048], P('cfg', None, 'dp', 'seq'), may hold values from -6 to 6
- hidden: bfloat16 [2, 2, 1024, 3072], P('cfg', 'dp', 'seq'), may hold values from -6 to 6
- adapter_down_weight: bfloat16 [3, 3072, 128], replicated, may hold values from -0.109375 to 0.109375
- adapter_up_weight: bfloat16 [3, 128, 2048], replicated, may hold values from -0.5 to 0.5
- guidance_index: int32 [2, 2], P(None, 'dp'), may hold values from 0 to 7
- timestep_index: int32 [2, 2], P(None, 'dp'), may hold values from 0 to 999
Outputs:
- student_out: bfloat16 [2, 2, 1024, 2048], P('cfg', 'dp', 'seq')
- grad_down: float32 [3, 3072, 128], P(None, ('cfg', 'seq', 'dp'))
- grad_up: float32 [3, 128, 2048], P(None, ('cfg', 'dp'), 'seq')
The draws below stay inside these ranges and needn't reach their ends.
All inputs are finite; a program needn't handle non-finite values.
Results may differ from the reference program's by a relative error of at most 0.02.
The reference program's roundings to bfloat16 on the way count: a program that leaves them out, or rounds other values in their place, can miss the bound.
Values may be sent and summed in bfloat16 or wider, within the bound.
A program may use at most 128 MiB of HBM per device.

```python
import math
import jax
import jax.numpy as jnp
from jax import lax

MODEL_WIDTH = 3072
HEADS = 16
HDIM = 128
ADAPTER_RANK = 128
GUIDES = 8
TSTEPS = 1000
ALL_HEADS_WIDTH = 2048
TOKENS = 1024
N_DP = 2


def field_shape():
    return (2, 2, N_DP, TOKENS, HEADS * HDIM)


def draw_teacher_query(key, part):
    field = 2.7 * jax.random.truncated_normal(jax.random.fold_in(key, 11), -2.2, 2.2, field_shape(), jnp.float32)
    return field.astype(jnp.bfloat16)


def draw_teacher_key(key, part):
    field = 2.7 * jax.random.truncated_normal(jax.random.fold_in(key, 23), -2.2, 2.2, field_shape(), jnp.float32)
    return field.astype(jnp.bfloat16)


def place_ends(entries, own_key, least, largest):
    longest = entries.shape.index(max(entries.shape))
    spots = []
    for shift in (0, 1):
        where = [jax.random.randint(jax.random.fold_in(own_key, axis), (), 0, length) for axis, length in enumerate(entries.shape)]
        where[longest] = (where[longest] + shift) % entries.shape[longest]
        spots.append(tuple(where))
    return entries.at[spots[0]].set(least).at[spots[1]].set(largest)


def with_spikes(values, own_key, source, target, parts, factor):
    owner, partner = [(jnp.arange(values.shape[dim]) // (values.shape[dim] // parts)).reshape([-1 if axis == dim else 1 for axis in range(values.ndim)]) for dim in (source, target)]
    chosen = jax.random.permutation(own_key, parts)[partner]
    strong = (owner == chosen) | (owner == (partner + parts // 2) % parts)
    return jnp.where(strong, factor * values, values)


def block_scale(rng, shape, split, low, high):
    gain = 1.0
    for dim, blocks in split:
        draws = jax.random.uniform(jax.random.fold_in(jax.random.fold_in(rng, 6), dim), (blocks,), jnp.float32, low / len(split), high / len(split))
        gain = gain * jnp.repeat(jnp.exp(draws), shape[dim] // blocks).reshape((-1,) + (1,) * (len(shape) - 1 - dim))
    return gain


def noise(rng, shape, width, most, shards=(), held_as=jnp.bfloat16):
    result = jax.random.normal(rng, shape, jnp.float32) * width
    if len(shards) > 0:
        result = block_scale(rng, shape, shards, -0.22, 0.18) * result
    return jnp.clip(result, min=-most, max=most).astype(held_as)


def noise_with(own_key, shape, spread, bound, cuts, heavy, dtype=jnp.bfloat16):
    values = spread * jax.random.normal(own_key, shape, jnp.float32)
    if cuts:
        values = values * block_scale(own_key, shape, cuts, -0.22, 0.18)
    return jnp.clip(with_spikes(values, jax.random.fold_in(own_key, 3), *heavy), -bound, bound).astype(dtype)


def setup_inputs(seed: int = 0) -> dict:
    streams_of = jax.random.split(jax.random.key(seed), 9)
    return {
        "teacher_query": draw_teacher_query(jax.random.fold_in(streams_of[8], 71), 0),
        "teacher_key": draw_teacher_key(jax.random.fold_in(streams_of[8], 71), 0),
        "teacher_value": noise(streams_of[2], (2, 2, N_DP, TOKENS, ALL_HEADS_WIDTH), 1.0, 6.0, ((0, 2), (2, 2), (3, 8))),
        "hidden": noise_with(streams_of[3], (2, N_DP, TOKENS, MODEL_WIDTH), 1.0, 6.0, ((0, 2), (1, 2), (2, 8)), (2, 3, 8, 2.0)),
        "adapter_down_weight": noise(streams_of[4], (3, MODEL_WIDTH, ADAPTER_RANK), MODEL_WIDTH ** -0.5, 0.109375),
        "adapter_up_weight": noise(streams_of[5], (3, ADAPTER_RANK, ALL_HEADS_WIDTH), ADAPTER_RANK ** -0.5, 0.5),
        "guidance_index": place_ends(jax.random.randint(streams_of[6], (2, N_DP), 0, GUIDES), jax.random.fold_in(streams_of[6], 1), 0, GUIDES - 1).astype(jnp.int32),
        "timestep_index": place_ends(jax.random.randint(streams_of[7], (2, N_DP), 0, TSTEPS), jax.random.fold_in(streams_of[7], 1), 0, TSTEPS - 1).astype(jnp.int32),
    }


def head_probs(query_head, key_head):
    scores = jnp.dot(query_head, key_head.T, preferred_element_type=jnp.float32) * HDIM ** (-0.5)
    highest = lax.optimization_barrier(jnp.max(scores, axis=-1, keepdims=True))
    raised = jnp.exp(scores - highest)
    return raised / lax.optimization_barrier(jnp.sum(raised, axis=-1, keepdims=True))

def to_heads(array):
    return array.reshape(array.shape[0], HEADS, HDIM).transpose(1, 0, 2)

def from_heads(array):
    return array.transpose(1, 0, 2).reshape(array.shape[1], HEADS * HDIM)

def attend(queries, keys, values):

    def per_head(triple):
        query_head, key_head, value_head = triple
        weights = head_probs(query_head, key_head).astype(jnp.bfloat16)
        return jnp.dot(weights, value_head, preferred_element_type=jnp.float32)
    return from_heads(lax.map(per_head, (to_heads(queries), to_heads(keys), to_heads(values))))

def attend_back(queries, keys, values, upstream):
    factor = HDIM ** (-0.5)

    def per_head(group):
        query_head, key_head, value_head, upstream_head = group
        probability = head_probs(query_head, key_head)
        weights = probability.astype(jnp.bfloat16)
        value_grad = jnp.dot(weights.T, upstream_head, preferred_element_type=jnp.float32)
        prob_grad = jnp.dot(upstream_head, value_head.T, preferred_element_type=jnp.float32)
        center = lax.optimization_barrier(jnp.sum(probability * prob_grad, axis=-1, keepdims=True))
        score_grad = (probability * (prob_grad - center)).astype(jnp.bfloat16)
        query_grad = jnp.dot(score_grad, key_head, preferred_element_type=jnp.float32) * factor
        key_grad = jnp.dot(score_grad.T, query_head, preferred_element_type=jnp.float32) * factor
        return (query_grad.astype(jnp.bfloat16), key_grad.astype(jnp.bfloat16), value_grad.astype(jnp.bfloat16))
    results = lax.map(per_head, (to_heads(queries), to_heads(keys), to_heads(values), to_heads(upstream)))
    return tuple((from_heads(stack_member) for stack_member in results))

def flatten(array):
    return array.reshape(-1, TOKENS, ALL_HEADS_WIDTH)

def reference(teacher_query, teacher_key, teacher_value, hidden, adapter_down_weight, adapter_up_weight, guidance_index, timestep_index):
    teacher_out = lax.map(lambda triple: attend(*triple).astype(jnp.bfloat16), (flatten(teacher_query), flatten(teacher_key), flatten(teacher_value)))
    teacher_out = teacher_out.reshape(2, 2, N_DP, TOKENS, ALL_HEADS_WIDTH).astype(jnp.float32)
    guide_scale = 1.0 + 0.5 * guidance_index.astype(jnp.float32)
    time_frac = (timestep_index.astype(jnp.float32) + 0.5) / TSTEPS
    target = teacher_out[1] + guide_scale[:, :, None, None] * (teacher_out[0] - teacher_out[1])
    rank_index = jnp.arange(1, ADAPTER_RANK + 1).astype(jnp.float32)
    feature_modulation = 1.0 + 0.5 * jnp.cos(math.pi * rank_index * time_frac[:, :, None] + 0.25 * rank_index * guide_scale[:, :, None])
    hidden_full_width = hidden.astype(jnp.float32)
    rank_projected = (jnp.einsum('eyog,mgf->meyof', hidden_full_width, adapter_down_weight.astype(jnp.float32)) * feature_modulation[None, :, :, None, :]).astype(jnp.bfloat16)
    up_full_width = adapter_up_weight.astype(jnp.float32)
    frozen = (teacher_query[0], teacher_key[0], teacher_value[0])
    student = []
    for stack_member in range(3):
        adapted_output = jnp.einsum('citr,rh->cith', rank_projected[stack_member].astype(jnp.float32), up_full_width[stack_member])
        student.append(flatten((frozen[stack_member].astype(jnp.float32) + adapted_output).astype(jnp.bfloat16)))
    student = tuple(student)
    student_flat = lax.map(lambda triple: attend(*triple).astype(jnp.bfloat16), student)
    student_out = student_flat.reshape(2, N_DP, TOKENS, ALL_HEADS_WIDTH)
    upstream = ((student_out.astype(jnp.float32) - target) * (1.0 / math.sqrt(2 * N_DP * TOKENS))).astype(jnp.bfloat16)
    grads = lax.map(lambda group: attend_back(*group), student + (flatten(upstream),))
    gradient_stack = jnp.stack(grads).astype(jnp.float32).reshape(3, 2, N_DP, TOKENS, ALL_HEADS_WIDTH)
    grad_up = jnp.einsum('kcitr,kcith->krh', rank_projected.astype(jnp.float32), gradient_stack)
    rank_backward = jnp.einsum('kcith,krh->kcitr', gradient_stack, up_full_width)
    low_grad = (rank_backward * feature_modulation[None, :, :, None, :]).astype(jnp.bfloat16)
    grad_down = jnp.einsum('citd,kcitr->kdr', hidden_full_width, low_grad.astype(jnp.float32))
    return (student_out, grad_down, grad_up)
```

```python
import functools
import math

import jax
import jax.numpy as jnp
from jax import lax
from jax.experimental import pallas as pl
from jax.experimental.pallas import tpu as pltpu
from jax.sharding import PartitionSpec as P

HDIM = 128
ADAPTER_RANK = 128
TSTEPS = 1000
FACTOR = HDIM ** (-0.5)
FACTOR_BASE2 = FACTOR * math.log2(math.e)
VMEM_LIMIT = 48 * 1024 * 1024

NT = (((1,), (1,)), ((), ()))
TN = (((0,), (0,)), ((), ()))


def dot_f32(left, right):
    return jnp.dot(left, right, preferred_element_type=jnp.float32)


def dot_nt(left, right):
    return lax.dot_general(left, right, NT, preferred_element_type=jnp.float32)


def probs_by_key(key_head, query_block):
    scores = dot_nt(key_head, query_block)
    highest = jnp.max(scores, axis=0, keepdims=True)
    raised = jnp.exp2((scores - highest) * FACTOR_BASE2)
    return raised * (1.0 / jnp.sum(raised, axis=0, keepdims=True))


def teacher_kernel(step_rows, half_ref, weight_ref, query_ref, key_ref, value_ref, out_ref, value_t):
    length = query_ref.shape[1]
    weight = weight_ref[0]
    value_t[...] = value_ref[0].T

    def one_block(step, _):
        rows = pl.ds(pl.multiple_of(step * step_rows, step_rows), step_rows)
        weights = probs_by_key(key_ref[0], query_ref[0, rows, :]).astype(jnp.bfloat16)
        attended = dot_f32(value_t[...], weights).T.astype(jnp.bfloat16)
        out_ref[rows, :] = (weight * attended.astype(jnp.float32)).astype(jnp.bfloat16)
        return 0

    lax.fori_loop(0, length // step_rows, one_block, 0)


def teacher_attention(half, weight, heads):
    _, length, columns = heads[0].shape
    heads_here = columns // HDIM
    step_rows = min(256, length)
    block = pl.BlockSpec((1, length, HDIM), lambda head, half_ref, weight_ref: (half_ref[0], 0, head))
    return pl.pallas_call(
        functools.partial(teacher_kernel, step_rows),
        out_shape=jax.ShapeDtypeStruct((length, columns), jnp.bfloat16),
        grid_spec=pltpu.PrefetchScalarGridSpec(
            num_scalar_prefetch=2,
            grid=(heads_here,),
            in_specs=[block, block, block],
            out_specs=pl.BlockSpec((length, HDIM), lambda head, half_ref, weight_ref: (0, head)),
            scratch_shapes=[pltpu.VMEM((HDIM, length), jnp.bfloat16)],
        ),
        compiler_params=pltpu.CompilerParams(
            dimension_semantics=("arbitrary",), vmem_limit_bytes=VMEM_LIMIT
        ),
        cost_estimate=pl.CostEstimate(
            flops=4 * heads_here * length * length * HDIM,
            bytes_accessed=8 * length * columns,
            transcendentals=heads_here * length * length,
        ),
        name="teacher",
    )(half[None], weight[None], *heads)


def student_kernel(
    step_rows,
    out_scale,
    cfg_ref,
    own_query,
    own_key,
    own_value,
    sent_query,
    sent_key,
    sent_value,
    rank_ref,
    up_ref,
    target_own,
    target_sent,
    out_ref,
    grad_up_ref,
    back_ref,
    s_query,
    s_key,
    s_value,
    key_t,
    value_t,
    grad_query,
    grad_key,
    grad_value,
    back_sum,
):
    length = rank_ref.shape[0]
    head = pl.program_id(0)
    first = cfg_ref[0] == 0

    for member, (own, sent, projected) in enumerate(
        ((own_query, sent_query, s_query), (own_key, sent_key, s_key), (own_value, sent_value, s_value))
    ):
        low_rank = rank_ref[:, member * ADAPTER_RANK : (member + 1) * ADAPTER_RANK]
        frozen = jnp.where(first, own[0].astype(jnp.float32), sent[...].astype(jnp.float32))
        projected[...] = (frozen + dot_f32(low_rank, up_ref[member])).astype(jnp.bfloat16)
    key_t[...] = s_key[...].T
    value_t[...] = s_value[...].T
    grad_key[...] = jnp.zeros_like(grad_key)
    grad_value[...] = jnp.zeros_like(grad_value)

    def one_block(step, _):
        rows = pl.ds(pl.multiple_of(step * step_rows, step_rows), step_rows)
        query_block = s_query[rows, :]
        probability = probs_by_key(s_key[...], query_block)
        weights = probability.astype(jnp.bfloat16)
        attended = dot_f32(value_t[...], weights).T.astype(jnp.bfloat16)
        out_ref[rows, :] = attended
        target = target_own[rows, :].astype(jnp.float32) + target_sent[rows, :].astype(jnp.float32)
        upstream = ((attended.astype(jnp.float32) - target) * out_scale).astype(jnp.bfloat16)
        grad_value[...] += dot_f32(weights, upstream)
        prob_grad = dot_nt(s_value[...], upstream)
        center = jnp.sum(probability * prob_grad, axis=0, keepdims=True)
        score_grad = (probability * (prob_grad - center)).astype(jnp.bfloat16)
        grad_key[...] += dot_f32(score_grad, query_block)
        grad_query[rows, :] = (dot_f32(key_t[...], score_grad).T * FACTOR).astype(jnp.bfloat16)
        return 0

    lax.fori_loop(0, length // step_rows, one_block, 0)

    gradients = (
        grad_query[...],
        (grad_key[...] * FACTOR).astype(jnp.bfloat16),
        grad_value[...].astype(jnp.bfloat16),
    )
    for member, gradient in enumerate(gradients):
        columns = slice(member * ADAPTER_RANK, (member + 1) * ADAPTER_RANK)
        grad_up_ref[member] = lax.dot_general(
            rank_ref[:, columns], gradient, TN, preferred_element_type=jnp.float32
        ).astype(jnp.bfloat16)
        back = dot_nt(gradient, up_ref[member])

        @pl.when(head == 0)
        def _():
            back_sum[:, columns] = back

        @pl.when(head > 0)
        def _():
            back_sum[:, columns] += back

    @pl.when(head == pl.num_programs(0) - 1)
    def _():
        back_ref[...] = back_sum[...].astype(jnp.bfloat16)


def student_step(cfg_index, total_rows, own, sent, rank_all, up_here, target_own, target_sent):
    length, columns = target_own.shape
    heads_here = columns // HDIM
    step_rows = min(256, length)
    ranks = rank_all.shape[1]
    own_block = pl.BlockSpec((1, length, HDIM), lambda head, cfg_ref: (0, 0, head))
    block = pl.BlockSpec((length, HDIM), lambda head, cfg_ref: (0, head))
    whole = pl.BlockSpec((length, ranks), lambda head, cfg_ref: (0, 0))
    up_block = pl.BlockSpec((3, ADAPTER_RANK, HDIM), lambda head, cfg_ref: (0, 0, head))
    return pl.pallas_call(
        functools.partial(student_kernel, step_rows, 1.0 / math.sqrt(total_rows)),
        out_shape=(
            jax.ShapeDtypeStruct((length, columns), jnp.bfloat16),
            jax.ShapeDtypeStruct((3, ADAPTER_RANK, columns), jnp.bfloat16),
            jax.ShapeDtypeStruct((length, ranks), jnp.bfloat16),
        ),
        grid_spec=pltpu.PrefetchScalarGridSpec(
            num_scalar_prefetch=1,
            grid=(heads_here,),
            in_specs=[own_block] * 3 + [block] * 3 + [whole, up_block, block, block],
            out_specs=(block, up_block, whole),
            scratch_shapes=[
                pltpu.VMEM((length, HDIM), jnp.bfloat16),
                pltpu.VMEM((length, HDIM), jnp.bfloat16),
                pltpu.VMEM((length, HDIM), jnp.bfloat16),
                pltpu.VMEM((HDIM, length), jnp.bfloat16),
                pltpu.VMEM((HDIM, length), jnp.bfloat16),
                pltpu.VMEM((length, HDIM), jnp.bfloat16),
                pltpu.VMEM((length, HDIM), jnp.float32),
                pltpu.VMEM((length, HDIM), jnp.float32),
                pltpu.VMEM((length, ranks), jnp.float32),
            ],
        ),
        compiler_params=pltpu.CompilerParams(
            dimension_semantics=("arbitrary",), vmem_limit_bytes=VMEM_LIMIT
        ),
        cost_estimate=pl.CostEstimate(
            flops=12 * heads_here * length * length * HDIM,
            bytes_accessed=24 * length * columns,
            transcendentals=heads_here * length * length,
        ),
        name="student",
    )(cfg_index[None], *own, *sent, rank_all, up_here, target_own, target_sent)


def exchanged(blocks, axis):
    return lax.all_to_all(blocks, axis, split_axis=0, concat_axis=0, tiled=True)


def gathered(value, axis):
    count = lax.axis_size(axis)
    return exchanged(jnp.broadcast_to(value[None], (count,) + value.shape), axis)


def body(
    teacher_query,
    teacher_key,
    teacher_value,
    hidden,
    adapter_down_weight,
    adapter_up_weight,
    guidance_index,
    timestep_index,
):
    cfg_index = lax.axis_index("cfg")
    seq_index = lax.axis_index("seq")
    seq_count = lax.axis_size("seq")
    dp_count = lax.axis_size("dp")
    tok_here = hidden.shape[2]
    length = tok_here * seq_count
    total_rows = 2 * dp_count * length
    ranks = 3 * ADAPTER_RANK
    input_features = hidden[0, 0]
    model_width = input_features.shape[1]
    half_cols = model_width // (2 * seq_count)

    guide_scale = 1.0 + 0.5 * guidance_index[:, 0].astype(jnp.float32)
    time_frac = (timestep_index[:, 0].astype(jnp.float32) + 0.5) / TSTEPS
    own_scale = lax.dynamic_index_in_dim(guide_scale, cfg_index, 0, keepdims=False)
    own_time = lax.dynamic_index_in_dim(time_frac, cfg_index, 0, keepdims=False)
    weighting = jnp.where(cfg_index == 0, guide_scale, 1.0 - guide_scale)
    rank_index = jnp.arange(1, ADAPTER_RANK + 1).astype(jnp.float32)
    feature_modulation = 1.0 + 0.5 * jnp.cos(
        math.pi * rank_index * own_time + 0.25 * rank_index * own_scale
    )
    modulation = jnp.tile(feature_modulation, 3)[None]

    teacher_heads = []
    sent = []
    for field in (teacher_query, teacher_key, teacher_value):
        heads = lax.all_to_all(field[0, :, 0], "seq", split_axis=2, concat_axis=1, tiled=True)
        teacher_heads.append(heads)
        sent.append(lax.ppermute(heads[1], "cfg", [(0, 1)]))

    rank_projected = jnp.concatenate(
        [dot_f32(input_features, adapter_down_weight[member]) for member in range(3)], axis=1
    )
    rank_projected = (rank_projected * modulation).astype(jnp.bfloat16)
    rank_all = gathered(rank_projected, "seq").reshape(length, ranks)

    split_view = input_features.reshape(tok_here, 2, seq_count, half_cols)
    split_view = split_view.transpose(2, 0, 1, 3).reshape(seq_count, tok_here, 2 * half_cols)
    column_block = exchanged(split_view, "seq").reshape(length, 2 * half_cols)

    other = 1 - cfg_index
    other_weighted = teacher_attention(
        other, lax.dynamic_index_in_dim(weighting, other, 0, keepdims=False), teacher_heads
    )
    target_sent = lax.ppermute(other_weighted, "cfg", [(0, 1), (1, 0)])
    target_own = teacher_attention(
        cfg_index, lax.dynamic_index_in_dim(weighting, cfg_index, 0, keepdims=False), teacher_heads
    )

    columns = target_own.shape[1]
    up_here = lax.dynamic_slice_in_dim(adapter_up_weight, seq_index * columns, columns, axis=2)
    student_local, up_partial, back_partial = student_step(
        cfg_index, total_rows, teacher_heads, sent, rank_all, up_here, target_own, target_sent
    )

    back_parts = exchanged(back_partial.reshape(seq_count, tok_here, ranks), "seq")
    rank_backward = jnp.sum(back_parts.astype(jnp.float32), axis=0)
    low_grad = (rank_backward * modulation).astype(jnp.bfloat16)
    student_tokens = lax.all_to_all(student_local, "seq", split_axis=0, concat_axis=1, tiled=True)
    grad_rows = gathered(low_grad, "seq").reshape(length, ranks)

    groups = 2 * dp_count
    up_rows = ADAPTER_RANK // groups
    up_parts = up_partial.reshape(3, groups, up_rows, columns).transpose(1, 0, 2, 3)
    grad_up = jnp.sum(exchanged(up_parts, ("cfg", "dp")).astype(jnp.float32), axis=0)

    column_partial = lax.dot_general(
        column_block, grad_rows, TN, preferred_element_type=jnp.float32
    ).astype(jnp.bfloat16)
    down_rows = 2 * half_cols // groups
    down_parts = exchanged(column_partial.reshape(groups, down_rows, ranks), ("cfg", "dp"))
    grad_down = jnp.sum(down_parts.astype(jnp.float32), axis=0)
    grad_down = grad_down.reshape(down_rows, 3, ADAPTER_RANK).transpose(1, 0, 2)
    return (student_tokens[None, None], grad_down, grad_up)


def solution(mesh):
    placed = (
        P("cfg", None, "dp", "seq", None),
        P("cfg", None, "dp", "seq", None),
        P("cfg", None, "dp", "seq", None),
        P("cfg", "dp", "seq", None),
        P(),
        P(),
        P(None, "dp"),
        P(None, "dp"),
    )
    return jax.shard_map(
        body,
        mesh=mesh,
        in_specs=placed,
        out_specs=(
            P("cfg", "dp", "seq", None),
            P(None, ("cfg", "seq", "dp"), None),
            P(None, ("cfg", "dp"), "seq"),
        ),
        check_vma=False,
    )
```

```python
import functools
import math

import jax
import jax.numpy as jnp
from jax import lax
from jax.experimental import pallas as pl
from jax.experimental.pallas import tpu as pltpu
from jax.sharding import PartitionSpec as P


HDIM = 128
ADAPTER_RANK = 128
TSTEPS = 1000
FACTOR = HDIM ** (-0.5)
FACTOR_BASE2 = FACTOR * math.log2(math.e)
VMEM_LIMIT = 48 * 1024 * 1024

NT = (((1,), (1,)), ((), ()))
TN = (((0,), (0,)), ((), ()))


def dot_f32(left, right):
    return jnp.dot(left, right, preferred_element_type=jnp.float32)


def dot_nt(left, right):
    return lax.dot_general(left, right, NT, preferred_element_type=jnp.float32)


def probs_by_key(key_head, query_block):
    scores = dot_nt(key_head, query_block)
    highest = jnp.max(scores, axis=0, keepdims=True)
    raised = jnp.exp2((scores - highest) * FACTOR_BASE2)
    return raised * (1.0 / jnp.sum(raised, axis=0, keepdims=True))


def teacher_kernel(step_rows, half_ref, weight_ref, query_ref, key_ref, value_ref, out_ref, value_t):
    length = query_ref.shape[1]
    weight = weight_ref[0]
    value_t[...] = value_ref[0].T

    def one_block(step, _):
        rows = pl.ds(pl.multiple_of(step * step_rows, step_rows), step_rows)
        weights = probs_by_key(key_ref[0], query_ref[0, rows, :]).astype(jnp.bfloat16)
        attended = dot_f32(value_t[...], weights).T.astype(jnp.bfloat16)
        out_ref[rows, :] = (weight * attended.astype(jnp.float32)).astype(jnp.bfloat16)
        return 0

    lax.fori_loop(0, length // step_rows, one_block, 0)


def teacher_attention(half, weight, heads):
    _, length, columns = heads[0].shape
    heads_here = columns // HDIM
    step_rows = min(256, length)
    block = pl.BlockSpec((1, length, HDIM), lambda head, half_ref, weight_ref: (half_ref[0], 0, head))
    return pl.pallas_call(
        functools.partial(teacher_kernel, step_rows),
        out_shape=jax.ShapeDtypeStruct((length, columns), jnp.bfloat16),
        grid_spec=pltpu.PrefetchScalarGridSpec(
            num_scalar_prefetch=2,
            grid=(heads_here,),
            in_specs=[block, block, block],
            out_specs=pl.BlockSpec((length, HDIM), lambda head, half_ref, weight_ref: (0, head)),
            scratch_shapes=[pltpu.VMEM((HDIM, length), jnp.bfloat16)],
        ),
        compiler_params=pltpu.CompilerParams(
            dimension_semantics=("arbitrary",), vmem_limit_bytes=VMEM_LIMIT
        ),
        cost_estimate=pl.CostEstimate(
            flops=4 * heads_here * length * length * HDIM,
            bytes_accessed=8 * length * columns,
            transcendentals=heads_here * length * length,
        ),
        name="teacher",
    )(half[None], weight[None], *heads)


def student_kernel(
    step_rows,
    out_scale,
    cfg_ref,
    own_query,
    own_key,
    own_value,
    sent_query,
    sent_key,
    sent_value,
    rank_ref,
    up_ref,
    target_own,
    target_sent,
    out_ref,
    grad_up_ref,
    back_ref,
    s_query,
    s_key,
    s_value,
    key_t,
    value_t,
    grad_query,
    grad_key,
    grad_value,
    back_sum,
):
    length = rank_ref.shape[0]
    head = pl.program_id(0)
    first = cfg_ref[0] == 0

    for member, (own, sent, projected) in enumerate(
        ((own_query, sent_query, s_query), (own_key, sent_key, s_key), (own_value, sent_value, s_value))
    ):
        low_rank = rank_ref[:, member * ADAPTER_RANK : (member + 1) * ADAPTER_RANK]
        frozen = jnp.where(first, own[0].astype(jnp.float32), sent[...].astype(jnp.float32))
        projected[...] = (frozen + dot_f32(low_rank, up_ref[member])).astype(jnp.bfloat16)
    key_t[...] = s_key[...].T
    value_t[...] = s_value[...].T
    grad_key[...] = jnp.zeros_like(grad_key)
    grad_value[...] = jnp.zeros_like(grad_value)

    def one_block(step, _):
        rows = pl.ds(pl.multiple_of(step * step_rows, step_rows), step_rows)
        query_block = s_query[rows, :]
        probability = probs_by_key(s_key[...], query_block)
        weights = probability.astype(jnp.bfloat16)
        attended = dot_f32(value_t[...], weights).T.astype(jnp.bfloat16)
        out_ref[rows, :] = attended
        target = target_own[rows, :].astype(jnp.float32) + target_sent[rows, :].astype(jnp.float32)
        upstream = ((attended.astype(jnp.float32) - target) * out_scale).astype(jnp.bfloat16)
        grad_value[...] += dot_f32(weights, upstream)
        prob_grad = dot_nt(s_value[...], upstream)
        center = jnp.sum(probability * prob_grad, axis=0, keepdims=True)
        score_grad = (probability * (prob_grad - center)).astype(jnp.bfloat16)
        grad_key[...] += dot_f32(score_grad, query_block)
        grad_query[rows, :] = (dot_f32(key_t[...], score_grad).T * FACTOR).astype(jnp.bfloat16)
        return 0

    lax.fori_loop(0, length // step_rows, one_block, 0)

    gradients = (
        grad_query[...],
        (grad_key[...] * FACTOR).astype(jnp.bfloat16),
        grad_value[...].astype(jnp.bfloat16),
    )
    for member, gradient in enumerate(gradients):
        columns = slice(member * ADAPTER_RANK, (member + 1) * ADAPTER_RANK)
        grad_up_ref[member] = lax.dot_general(
            rank_ref[:, columns], gradient, TN, preferred_element_type=jnp.float32
        ).astype(jnp.bfloat16)
        back = dot_nt(gradient, up_ref[member])

        @pl.when(head == 0)
        def _():
            back_sum[:, columns] = back

        @pl.when(head > 0)
        def _():
            back_sum[:, columns] += back

    @pl.when(head == pl.num_programs(0) - 1)
    def _():
        back_ref[...] = back_sum[...].astype(jnp.bfloat16)


def student_step(cfg_index, total_rows, own, sent, rank_all, up_here, target_own, target_sent):
    length, columns = target_own.shape
    heads_here = columns // HDIM
    step_rows = min(256, length)
    ranks = rank_all.shape[1]
    own_block = pl.BlockSpec((1, length, HDIM), lambda head, cfg_ref: (0, 0, head))
    block = pl.BlockSpec((length, HDIM), lambda head, cfg_ref: (0, head))
    whole = pl.BlockSpec((length, ranks), lambda head, cfg_ref: (0, 0))
    up_block = pl.BlockSpec((3, ADAPTER_RANK, HDIM), lambda head, cfg_ref: (0, 0, head))
    return pl.pallas_call(
        functools.partial(student_kernel, step_rows, 1.0 / math.sqrt(total_rows)),
        out_shape=(
            jax.ShapeDtypeStruct((length, columns), jnp.bfloat16),
            jax.ShapeDtypeStruct((3, ADAPTER_RANK, columns), jnp.bfloat16),
            jax.ShapeDtypeStruct((length, ranks), jnp.bfloat16),
        ),
        grid_spec=pltpu.PrefetchScalarGridSpec(
            num_scalar_prefetch=1,
            grid=(heads_here,),
            in_specs=[own_block] * 3 + [block] * 3 + [whole, up_block, block, block],
            out_specs=(block, up_block, whole),
            scratch_shapes=[
                pltpu.VMEM((length, HDIM), jnp.bfloat16),
                pltpu.VMEM((length, HDIM), jnp.bfloat16),
                pltpu.VMEM((length, HDIM), jnp.bfloat16),
                pltpu.VMEM((HDIM, length), jnp.bfloat16),
                pltpu.VMEM((HDIM, length), jnp.bfloat16),
                pltpu.VMEM((length, HDIM), jnp.bfloat16),
                pltpu.VMEM((length, HDIM), jnp.float32),
                pltpu.VMEM((length, HDIM), jnp.float32),
                pltpu.VMEM((length, ranks), jnp.float32),
            ],
        ),
        compiler_params=pltpu.CompilerParams(
            dimension_semantics=("arbitrary",), vmem_limit_bytes=VMEM_LIMIT
        ),
        cost_estimate=pl.CostEstimate(
            flops=12 * heads_here * length * length * HDIM,
            bytes_accessed=24 * length * columns,
            transcendentals=heads_here * length * length,
        ),
        name="student",
    )(cfg_index[None], *own, *sent, rank_all, up_here, target_own, target_sent)


def scatter_kernel(count, *refs):
    fields = refs[0:3]
    heads = refs[3:6]
    sent = refs[6:9]
    kept, send_sem, recv_sem, pass_send_sem, pass_recv_sem, load_sem, store_sem = refs[9:]
    me = lax.axis_index("seq")
    cfg_index = lax.axis_index("cfg")
    tok_here = fields[0].shape[1]
    columns = heads[0].shape[2]

    loads = []
    own_columns = pl.ds(pl.multiple_of(me * columns, columns), columns)
    own_rows = pl.ds(pl.multiple_of(me * tok_here, tok_here), tok_here)
    for member in range(3):
        load = pltpu.make_async_copy(
            fields[member].at[:, :, own_columns], kept.at[member], load_sem.at[member]
        )
        load.start()
        loads.append(load)

    barrier = pltpu.get_barrier_semaphore()
    for step in range(1, count):
        pl.semaphore_signal(
            barrier,
            inc=1,
            device_id={"seq": lax.rem(me + step, count)},
            device_id_type=pl.DeviceIdType.MESH,
        )
    pl.semaphore_signal(
        barrier, inc=1, device_id={"cfg": 1 - cfg_index}, device_id_type=pl.DeviceIdType.MESH
    )
    pl.semaphore_wait(barrier, count)

    def scattered(member, step):
        peer = lax.rem(me + step, count)
        peer_columns = pl.ds(pl.multiple_of(peer * columns, columns), columns)
        return pltpu.make_async_remote_copy(
            src_ref=fields[member].at[:, :, peer_columns],
            dst_ref=heads[member].at[:, own_rows, :],
            send_sem=send_sem.at[member, step],
            recv_sem=recv_sem.at[member, step],
            device_id={"seq": peer},
            device_id_type=pl.DeviceIdType.MESH,
        )

    def passed(member, step):
        source = lax.rem(me - step + count, count)
        rows = pl.ds(pl.multiple_of(source * tok_here, tok_here), tok_here)
        block = kept.at[member, 1] if step == 0 else heads[member].at[1, rows, :]
        return pltpu.make_async_remote_copy(
            src_ref=block,
            dst_ref=sent[member].at[rows, :],
            send_sem=pass_send_sem.at[member, step],
            recv_sem=pass_recv_sem.at[member, step],
            device_id={"cfg": 1 - cfg_index},
            device_id_type=pl.DeviceIdType.MESH,
        )

    for member in range(3):
        for step in range(1, count):
            scattered(member, step).start()

    stores = []
    for member in range(3):
        loads[member].wait()
        store = pltpu.make_async_copy(
            kept.at[member], heads[member].at[:, own_rows, :], store_sem.at[member]
        )
        store.start()
        stores.append(store)

    for member in range(3):
        for step in range(count):
            if step > 0:
                scattered(member, step).wait_recv()

            @pl.when(cfg_index == 0)
            def _():
                passed(member, step).start()

    for member in range(3):
        stores[member].wait()
        for step in range(count):
            if step > 0:
                scattered(member, step).wait_send()

            @pl.when(cfg_index == 0)
            def _():
                passed(member, step).wait_send()

            @pl.when(cfg_index == 1)
            def _():
                passed(member, step).wait_recv()


def scatter_teacher(fields):
    count = lax.axis_size("seq")
    halves, tok_here, width = fields[0].shape
    length, columns = tok_here * count, width // count
    any_spec = pl.BlockSpec(memory_space=pl.ANY)
    outs = pl.pallas_call(
        functools.partial(scatter_kernel, count),
        out_shape=[jax.ShapeDtypeStruct((halves, length, columns), jnp.bfloat16)] * 3
        + [jax.ShapeDtypeStruct((length, columns), jnp.bfloat16)] * 3,
        in_specs=[any_spec] * 3,
        out_specs=[any_spec] * 6,
        scratch_shapes=[
            pltpu.VMEM((3, halves, tok_here, columns), jnp.bfloat16),
            pltpu.SemaphoreType.DMA((3, count)),
            pltpu.SemaphoreType.DMA((3, count)),
            pltpu.SemaphoreType.DMA((3, count)),
            pltpu.SemaphoreType.DMA((3, count)),
            pltpu.SemaphoreType.DMA((3,)),
            pltpu.SemaphoreType.DMA((3,)),
        ],
        compiler_params=pltpu.CompilerParams(collective_id=0, has_side_effects=True),
        cost_estimate=pl.CostEstimate(
            flops=0, bytes_accessed=12 * halves * length * columns, transcendentals=0
        ),
        name="scatter",
    )(*fields)
    return outs[0:3], outs[3:6]


def exchanged(blocks, axis):
    return lax.all_to_all(blocks, axis, split_axis=0, concat_axis=0, tiled=True)


def gathered(value, axis):
    count = lax.axis_size(axis)
    return exchanged(jnp.broadcast_to(value[None], (count,) + value.shape), axis)


def body(
    teacher_query,
    teacher_key,
    teacher_value,
    hidden,
    adapter_down_weight,
    adapter_up_weight,
    guidance_index,
    timestep_index,
):
    cfg_index = lax.axis_index("cfg")
    seq_index = lax.axis_index("seq")
    seq_count = lax.axis_size("seq")
    dp_count = lax.axis_size("dp")
    tok_here = hidden.shape[2]
    length = tok_here * seq_count
    total_rows = 2 * dp_count * length
    ranks = 3 * ADAPTER_RANK
    input_features = hidden[0, 0]
    model_width = input_features.shape[1]
    half_cols = model_width // (2 * seq_count)

    guide_scale = 1.0 + 0.5 * guidance_index[:, 0].astype(jnp.float32)
    time_frac = (timestep_index[:, 0].astype(jnp.float32) + 0.5) / TSTEPS
    own_scale = lax.dynamic_index_in_dim(guide_scale, cfg_index, 0, keepdims=False)
    own_time = lax.dynamic_index_in_dim(time_frac, cfg_index, 0, keepdims=False)
    weighting = jnp.where(cfg_index == 0, guide_scale, 1.0 - guide_scale)
    rank_index = jnp.arange(1, ADAPTER_RANK + 1).astype(jnp.float32)
    feature_modulation = 1.0 + 0.5 * jnp.cos(
        math.pi * rank_index * own_time + 0.25 * rank_index * own_scale
    )
    modulation = jnp.tile(feature_modulation, 3)[None]

    teacher_heads, sent = scatter_teacher(
        (teacher_query[0, :, 0], teacher_key[0, :, 0], teacher_value[0, :, 0])
    )

    rank_projected = jnp.concatenate(
        [dot_f32(input_features, adapter_down_weight[member]) for member in range(3)], axis=1
    )
    rank_projected = (rank_projected * modulation).astype(jnp.bfloat16)
    rank_projected, *teacher_heads = lax.optimization_barrier((rank_projected, *teacher_heads))
    rank_all = gathered(rank_projected, "seq")
    rank_all = rank_all.reshape(length, ranks)

    split_view = input_features.reshape(tok_here, 2, seq_count, half_cols)
    split_view, rank_all = lax.optimization_barrier((split_view, rank_all))
    split_view = split_view.transpose(2, 0, 1, 3).reshape(seq_count, tok_here, 2 * half_cols)
    column_block = exchanged(split_view, "seq")
    column_block = column_block.reshape(length, 2 * half_cols)

    other = 1 - cfg_index
    other_weighted = teacher_attention(
        other, lax.dynamic_index_in_dim(weighting, other, 0, keepdims=False), teacher_heads
    )
    target_sent = lax.ppermute(other_weighted, "cfg", [(0, 1), (1, 0)])
    target_own = teacher_attention(
        cfg_index,
        lax.dynamic_index_in_dim(weighting, cfg_index, 0, keepdims=False),
        teacher_heads,
    )

    columns = target_own.shape[1]
    up_here = lax.dynamic_slice_in_dim(adapter_up_weight, seq_index * columns, columns, axis=2)
    student_local, up_partial, back_partial = student_step(
        cfg_index, total_rows, teacher_heads, sent, rank_all, up_here, target_own, target_sent
    )

    student_local, up_partial, back_partial, column_block = lax.optimization_barrier(
        (student_local, up_partial, back_partial, column_block)
    )
    back_parts = exchanged(back_partial.reshape(seq_count, tok_here, ranks), "seq")
    rank_backward = jnp.sum(back_parts.astype(jnp.float32), axis=0)
    low_grad = (rank_backward * modulation).astype(jnp.bfloat16)
    student_tokens = lax.all_to_all(student_local, "seq", split_axis=0, concat_axis=1, tiled=True)
    grad_rows = gathered(low_grad, "seq").reshape(length, ranks)

    groups = 2 * dp_count
    up_rows = ADAPTER_RANK // groups
    up_parts = up_partial.reshape(3, groups, up_rows, columns).transpose(1, 0, 2, 3)
    grad_up = jnp.sum(exchanged(up_parts, ("cfg", "dp")).astype(jnp.float32), axis=0)

    column_partial = lax.dot_general(
        column_block, grad_rows, TN, preferred_element_type=jnp.float32
    ).astype(jnp.bfloat16)
    down_rows = 2 * half_cols // groups
    down_parts = exchanged(column_partial.reshape(groups, down_rows, ranks), ("cfg", "dp"))
    grad_down = jnp.sum(down_parts.astype(jnp.float32), axis=0)
    grad_down = grad_down.reshape(down_rows, 3, ADAPTER_RANK).transpose(1, 0, 2)
    return (student_tokens[None, None], grad_down, grad_up)


def solution(mesh):
    placed = (
        P("cfg", None, "dp", "seq", None),
        P("cfg", None, "dp", "seq", None),
        P("cfg", None, "dp", "seq", None),
        P("cfg", "dp", "seq", None),
        P(),
        P(),
        P(None, "dp"),
        P(None, "dp"),
    )
    return jax.shard_map(
        body,
        mesh=mesh,
        in_specs=placed,
        out_specs=(
            P("cfg", "dp", "seq", None),
            P(None, ("cfg", "seq", "dp"), None),
            P(None, ("cfg", "dp"), "seq"),
        ),
        check_vma=False,
    )
```

```python
import functools
import math

import jax
import jax.numpy as jnp
from jax import lax
from jax.experimental import pallas as pl
from jax.experimental.pallas import tpu as pltpu
from jax.sharding import PartitionSpec as P


HDIM = 128
ADAPTER_RANK = 128
TSTEPS = 1000
FACTOR = HDIM ** (-0.5)
FACTOR_BASE2 = FACTOR * math.log2(math.e)
VMEM_LIMIT = 60 * 1024 * 1024

NT = (((1,), (1,)), ((), ()))
TN = (((0,), (0,)), ((), ()))


def dot_f32(left, right):
    return jnp.dot(left, right, preferred_element_type=jnp.float32)


def dot_nt(left, right):
    return lax.dot_general(left, right, NT, preferred_element_type=jnp.float32)


def probs_by_key(key_head, query_block):
    scores = dot_nt(key_head, query_block)
    highest = jnp.max(scores, axis=0, keepdims=True)
    raised = jnp.exp2((scores - highest) * FACTOR_BASE2)
    return raised * (1.0 / jnp.sum(raised, axis=0, keepdims=True))


def teacher_kernel(step_rows, half_ref, weight_ref, query_ref, key_ref, value_ref, out_ref, value_t):
    length = query_ref.shape[1]
    weight = weight_ref[0]
    value_t[...] = value_ref[0].T

    def one_block(step, _):
        rows = pl.ds(pl.multiple_of(step * step_rows, step_rows), step_rows)
        weights = probs_by_key(key_ref[0], query_ref[0, rows, :]).astype(jnp.bfloat16)
        attended = dot_f32(value_t[...], weights).T.astype(jnp.bfloat16)
        out_ref[rows, :] = (weight * attended.astype(jnp.float32)).astype(jnp.bfloat16)
        return 0

    lax.fori_loop(0, length // step_rows, one_block, 0)


def teacher_attention(half, weight, heads):
    _, length, columns = heads[0].shape
    heads_here = columns // HDIM
    step_rows = min(256, length)
    block = pl.BlockSpec((1, length, HDIM), lambda head, half_ref, weight_ref: (half_ref[0], 0, head))
    return pl.pallas_call(
        functools.partial(teacher_kernel, step_rows),
        out_shape=jax.ShapeDtypeStruct((length, columns), jnp.bfloat16),
        grid_spec=pltpu.PrefetchScalarGridSpec(
            num_scalar_prefetch=2,
            grid=(heads_here,),
            in_specs=[block, block, block],
            out_specs=pl.BlockSpec((length, HDIM), lambda head, half_ref, weight_ref: (0, head)),
            scratch_shapes=[pltpu.VMEM((HDIM, length), jnp.bfloat16)],
        ),
        compiler_params=pltpu.CompilerParams(
            dimension_semantics=("arbitrary",), vmem_limit_bytes=VMEM_LIMIT
        ),
        cost_estimate=pl.CostEstimate(
            flops=4 * heads_here * length * length * HDIM,
            bytes_accessed=8 * length * columns,
            transcendentals=heads_here * length * length,
        ),
        name="teacher",
    )(half[None], weight[None], *heads)


def student_kernel(
    step_rows,
    out_scale,
    cfg_ref,
    own_query,
    own_key,
    own_value,
    sent_query,
    sent_key,
    sent_value,
    rank_ref,
    up_ref,
    target_own,
    target_sent,
    out_ref,
    grad_up_ref,
    back_ref,
    s_query,
    s_key,
    s_value,
    key_t,
    value_t,
    grad_query,
    grad_key,
    grad_value,
    back_sum,
):
    length = rank_ref.shape[0]
    head = pl.program_id(0)
    first = cfg_ref[0] == 0

    for member, (own, sent, projected) in enumerate(
        ((own_query, sent_query, s_query), (own_key, sent_key, s_key), (own_value, sent_value, s_value))
    ):
        low_rank = rank_ref[:, member * ADAPTER_RANK : (member + 1) * ADAPTER_RANK]
        frozen = jnp.where(first, own[0].astype(jnp.float32), sent[...].astype(jnp.float32))
        projected[...] = (frozen + dot_f32(low_rank, up_ref[member])).astype(jnp.bfloat16)
    key_t[...] = s_key[...].T
    value_t[...] = s_value[...].T
    grad_key[...] = jnp.zeros_like(grad_key)
    grad_value[...] = jnp.zeros_like(grad_value)

    def one_block(step, _):
        rows = pl.ds(pl.multiple_of(step * step_rows, step_rows), step_rows)
        query_block = s_query[rows, :]
        probability = probs_by_key(s_key[...], query_block)
        weights = probability.astype(jnp.bfloat16)
        attended = dot_f32(value_t[...], weights).T.astype(jnp.bfloat16)
        out_ref[rows, :] = attended
        target = target_own[rows, :].astype(jnp.float32) + target_sent[rows, :].astype(jnp.float32)
        upstream = ((attended.astype(jnp.float32) - target) * out_scale).astype(jnp.bfloat16)
        grad_value[...] += dot_f32(weights, upstream)
        prob_grad = dot_nt(s_value[...], upstream)
        center = jnp.sum(probability * prob_grad, axis=0, keepdims=True)
        score_grad = (probability * (prob_grad - center)).astype(jnp.bfloat16)
        grad_key[...] += dot_f32(score_grad, query_block)
        grad_query[rows, :] = (dot_f32(key_t[...], score_grad).T * FACTOR).astype(jnp.bfloat16)
        return 0

    lax.fori_loop(0, length // step_rows, one_block, 0)

    gradients = (
        grad_query[...],
        (grad_key[...] * FACTOR).astype(jnp.bfloat16),
        grad_value[...].astype(jnp.bfloat16),
    )
    for member, gradient in enumerate(gradients):
        columns = slice(member * ADAPTER_RANK, (member + 1) * ADAPTER_RANK)
        grad_up_ref[member] = lax.dot_general(
            rank_ref[:, columns], gradient, TN, preferred_element_type=jnp.float32
        ).astype(jnp.bfloat16)
        back = dot_nt(gradient, up_ref[member])

        @pl.when(head == 0)
        def _():
            back_sum[:, columns] = back

        @pl.when(head > 0)
        def _():
            back_sum[:, columns] += back

    @pl.when(head == pl.num_programs(0) - 1)
    def _():
        back_ref[...] = back_sum[...].astype(jnp.bfloat16)


def student_step(cfg_index, total_rows, own, sent, rank_all, up_here, target_own, target_sent):
    length, columns = target_own.shape
    heads_here = columns // HDIM
    step_rows = min(256, length)
    ranks = rank_all.shape[1]
    own_block = pl.BlockSpec((1, length, HDIM), lambda head, cfg_ref: (0, 0, head))
    block = pl.BlockSpec((length, HDIM), lambda head, cfg_ref: (0, head))
    whole = pl.BlockSpec((length, ranks), lambda head, cfg_ref: (0, 0))
    up_block = pl.BlockSpec((3, ADAPTER_RANK, HDIM), lambda head, cfg_ref: (0, 0, head))
    return pl.pallas_call(
        functools.partial(student_kernel, step_rows, 1.0 / math.sqrt(total_rows)),
        out_shape=(
            jax.ShapeDtypeStruct((length, columns), jnp.bfloat16),
            jax.ShapeDtypeStruct((3, ADAPTER_RANK, columns), jnp.bfloat16),
            jax.ShapeDtypeStruct((length, ranks), jnp.bfloat16),
        ),
        grid_spec=pltpu.PrefetchScalarGridSpec(
            num_scalar_prefetch=1,
            grid=(heads_here,),
            in_specs=[own_block] * 3 + [block] * 3 + [whole, up_block, block, block],
            out_specs=(block, up_block, whole),
            scratch_shapes=[
                pltpu.VMEM((length, HDIM), jnp.bfloat16),
                pltpu.VMEM((length, HDIM), jnp.bfloat16),
                pltpu.VMEM((length, HDIM), jnp.bfloat16),
                pltpu.VMEM((HDIM, length), jnp.bfloat16),
                pltpu.VMEM((HDIM, length), jnp.bfloat16),
                pltpu.VMEM((length, HDIM), jnp.bfloat16),
                pltpu.VMEM((length, HDIM), jnp.float32),
                pltpu.VMEM((length, HDIM), jnp.float32),
                pltpu.VMEM((length, ranks), jnp.float32),
            ],
        ),
        compiler_params=pltpu.CompilerParams(
            dimension_semantics=("arbitrary",), vmem_limit_bytes=VMEM_LIMIT
        ),
        cost_estimate=pl.CostEstimate(
            flops=12 * heads_here * length * length * HDIM,
            bytes_accessed=24 * length * columns,
            transcendentals=heads_here * length * length,
        ),
        name="student",
    )(cfg_index[None], *own, *sent, rank_all, up_here, target_own, target_sent)


def scatter_kernel(count, *refs):
    fields = refs[0:3]
    heads = refs[3:6]
    sent = refs[6:9]
    kept, send_sem, recv_sem, pass_send_sem, pass_recv_sem, load_sem, store_sem = refs[9:]
    me = lax.axis_index("seq")
    cfg_index = lax.axis_index("cfg")
    tok_here = fields[0].shape[1]
    columns = heads[0].shape[2]

    loads = []
    own_columns = pl.ds(pl.multiple_of(me * columns, columns), columns)
    own_rows = pl.ds(pl.multiple_of(me * tok_here, tok_here), tok_here)
    for member in range(3):
        load = pltpu.make_async_copy(
            fields[member].at[:, :, own_columns], kept.at[member], load_sem.at[member]
        )
        load.start()
        loads.append(load)

    barrier = pltpu.get_barrier_semaphore()
    for step in range(1, count):
        pl.semaphore_signal(
            barrier,
            inc=1,
            device_id={"seq": lax.rem(me + step, count)},
            device_id_type=pl.DeviceIdType.MESH,
        )
    pl.semaphore_signal(
        barrier, inc=1, device_id={"cfg": 1 - cfg_index}, device_id_type=pl.DeviceIdType.MESH
    )
    pl.semaphore_wait(barrier, count)

    def scattered(member, step):
        peer = lax.rem(me + step, count)
        peer_columns = pl.ds(pl.multiple_of(peer * columns, columns), columns)
        return pltpu.make_async_remote_copy(
            src_ref=fields[member].at[:, :, peer_columns],
            dst_ref=heads[member].at[:, own_rows, :],
            send_sem=send_sem.at[member, step],
            recv_sem=recv_sem.at[member, step],
            device_id={"seq": peer},
            device_id_type=pl.DeviceIdType.MESH,
        )

    def passed(member, step):
        source = lax.rem(me - step + count, count)
        rows = pl.ds(pl.multiple_of(source * tok_here, tok_here), tok_here)
        block = kept.at[member, 1] if step == 0 else heads[member].at[1, rows, :]
        return pltpu.make_async_remote_copy(
            src_ref=block,
            dst_ref=sent[member].at[rows, :],
            send_sem=pass_send_sem.at[member, step],
            recv_sem=pass_recv_sem.at[member, step],
            device_id={"cfg": 1 - cfg_index},
            device_id_type=pl.DeviceIdType.MESH,
        )

    for member in range(3):
        for step in range(1, count):
            scattered(member, step).start()

    stores = []
    for member in range(3):
        loads[member].wait()
        store = pltpu.make_async_copy(
            kept.at[member], heads[member].at[:, own_rows, :], store_sem.at[member]
        )
        store.start()
        stores.append(store)

    for member in range(3):
        for step in range(count):
            if step > 0:
                scattered(member, step).wait_recv()

            @pl.when(cfg_index == 0)
            def _():
                passed(member, step).start()

    for member in range(3):
        stores[member].wait()
        for step in range(count):
            if step > 0:
                scattered(member, step).wait_send()

            @pl.when(cfg_index == 0)
            def _():
                passed(member, step).wait_send()

            @pl.when(cfg_index == 1)
            def _():
                passed(member, step).wait_recv()


def scatter_teacher(fields):
    count = lax.axis_size("seq")
    halves, tok_here, width = fields[0].shape
    length, columns = tok_here * count, width // count
    any_spec = pl.BlockSpec(memory_space=pl.ANY)
    outs = pl.pallas_call(
        functools.partial(scatter_kernel, count),
        out_shape=[jax.ShapeDtypeStruct((halves, length, columns), jnp.bfloat16)] * 3
        + [jax.ShapeDtypeStruct((length, columns), jnp.bfloat16)] * 3,
        in_specs=[any_spec] * 3,
        out_specs=[any_spec] * 6,
        scratch_shapes=[
            pltpu.VMEM((3, halves, tok_here, columns), jnp.bfloat16),
            pltpu.SemaphoreType.DMA((3, count)),
            pltpu.SemaphoreType.DMA((3, count)),
            pltpu.SemaphoreType.DMA((3, count)),
            pltpu.SemaphoreType.DMA((3, count)),
            pltpu.SemaphoreType.DMA((3,)),
            pltpu.SemaphoreType.DMA((3,)),
        ],
        compiler_params=pltpu.CompilerParams(collective_id=0, has_side_effects=True),
        cost_estimate=pl.CostEstimate(
            flops=0, bytes_accessed=12 * halves * length * columns, transcendentals=0
        ),
        name="scatter",
    )(*fields)
    return outs[0:3], outs[3:6]


def tail_kernel(
    count,
    dp_count,
    back_ref,
    student_ref,
    up_ref,
    modulation_ref,
    tokens_ref,
    grad_up_ref,
    rows_ref,
    parts,
    up_parts,
    kept,
    mine,
    send_sem,
    recv_sem,
    up_send_sem,
    up_recv_sem,
    local_sem,
):
    me = lax.axis_index("seq")
    groups = 2 * dp_count
    group = lax.axis_index("cfg") * dp_count + lax.axis_index("dp")
    tok_here = mine.shape[0]
    columns = student_ref.shape[1]

    def rows_of(device):
        return pl.ds(pl.multiple_of(device * tok_here, tok_here), tok_here)

    own_columns = pl.ds(pl.multiple_of(me * columns, columns), columns)

    def group_device(step):
        peer = lax.rem(group + step, groups)
        return {"cfg": peer // dp_count, "dp": lax.rem(peer, dp_count)}

    own_loads = [
        pltpu.make_async_copy(back_ref.at[rows_of(me), :], parts.at[0], local_sem.at[0]),
        pltpu.make_async_copy(student_ref.at[rows_of(me), :], kept, local_sem.at[1]),
        pltpu.make_async_copy(up_ref.at[group], up_parts.at[0], local_sem.at[2]),
    ]
    for load in own_loads:
        load.start()

    barrier = pltpu.get_barrier_semaphore()
    for step in range(1, count):
        pl.semaphore_signal(
            barrier,
            inc=1,
            device_id={"seq": lax.rem(me + step, count)},
            device_id_type=pl.DeviceIdType.MESH,
        )
    for step in range(1, groups):
        pl.semaphore_signal(
            barrier, inc=1, device_id=group_device(step), device_id_type=pl.DeviceIdType.MESH
        )
    pl.semaphore_wait(barrier, count + groups - 2)

    def remote(kind, step):
        peer = lax.rem(me + step, count)
        source, target = (
            (back_ref.at[rows_of(peer), :], parts.at[step]),
            (student_ref.at[rows_of(peer), :], tokens_ref.at[:, own_columns]),
            (mine, rows_ref.at[rows_of(me), :]),
        )[kind]
        return pltpu.make_async_remote_copy(
            src_ref=source,
            dst_ref=target,
            send_sem=send_sem.at[kind, step],
            recv_sem=recv_sem.at[kind, step],
            device_id={"seq": peer},
            device_id_type=pl.DeviceIdType.MESH,
        )

    def up_remote(step):
        return pltpu.make_async_remote_copy(
            src_ref=up_ref.at[lax.rem(group + step, groups)],
            dst_ref=up_parts.at[step],
            send_sem=up_send_sem.at[step],
            recv_sem=up_recv_sem.at[step],
            device_id=group_device(step),
            device_id_type=pl.DeviceIdType.MESH,
        )

    for step in range(1, count):
        remote(0, step).start()
    for step in range(1, groups):
        up_remote(step).start()
    for step in range(1, count):
        remote(1, step).start()
    for load in own_loads:
        load.wait()
    own_store = pltpu.make_async_copy(kept, tokens_ref.at[:, own_columns], local_sem.at[3])
    own_store.start()

    total = parts[0].astype(jnp.float32)
    for step in range(1, count):
        remote(0, step).wait_recv()
        total = total + parts[step].astype(jnp.float32)
    low_grad = (total * modulation_ref[...]).astype(jnp.bfloat16)
    mine[...] = low_grad
    rows_ref[rows_of(me), :] = low_grad
    for step in range(1, count):
        remote(2, step).start()

    up_total = up_parts[0].astype(jnp.float32)
    for step in range(1, groups):
        up_remote(step).wait()
        up_total = up_total + up_parts[step].astype(jnp.float32)
    grad_up_ref[...] = up_total

    own_store.wait()
    for step in range(1, count):
        remote(0, step).wait_send()
        remote(1, step).wait()
        remote(2, step).wait()


def tail_exchange(back_partial, student_local, up_blocks, modulation):
    count = lax.axis_size("seq")
    dp_count = lax.axis_size("dp")
    length, ranks = back_partial.shape
    columns = student_local.shape[1]
    tok_here = length // count
    any_spec = pl.BlockSpec(memory_space=pl.ANY)
    vmem_spec = pl.BlockSpec(memory_space=pltpu.VMEM)
    return pl.pallas_call(
        functools.partial(tail_kernel, count, dp_count),
        out_shape=(
            jax.ShapeDtypeStruct((tok_here, columns * count), jnp.bfloat16),
            jax.ShapeDtypeStruct(up_blocks.shape[1:], jnp.float32),
            jax.ShapeDtypeStruct((length, ranks), jnp.bfloat16),
        ),
        in_specs=[any_spec, any_spec, any_spec, vmem_spec],
        out_specs=(any_spec, vmem_spec, vmem_spec),
        scratch_shapes=[
            pltpu.VMEM((count, tok_here, ranks), jnp.bfloat16),
            pltpu.VMEM(up_blocks.shape, jnp.bfloat16),
            pltpu.VMEM((tok_here, columns), jnp.bfloat16),
            pltpu.VMEM((tok_here, ranks), jnp.bfloat16),
            pltpu.SemaphoreType.DMA((3, count)),
            pltpu.SemaphoreType.DMA((3, count)),
            pltpu.SemaphoreType.DMA((2 * dp_count,)),
            pltpu.SemaphoreType.DMA((2 * dp_count,)),
            pltpu.SemaphoreType.DMA((4,)),
        ],
        compiler_params=pltpu.CompilerParams(collective_id=1, has_side_effects=True),
        cost_estimate=pl.CostEstimate(
            flops=0, bytes_accessed=8 * length * ranks, transcendentals=0
        ),
        name="tail",
    )(back_partial, student_local, up_blocks, modulation)


def exchanged(blocks, axis):
    return lax.all_to_all(blocks, axis, split_axis=0, concat_axis=0, tiled=True)


def gathered(value, axis):
    count = lax.axis_size(axis)
    return exchanged(jnp.broadcast_to(value[None], (count,) + value.shape), axis)


def body(
    teacher_query,
    teacher_key,
    teacher_value,
    hidden,
    adapter_down_weight,
    adapter_up_weight,
    guidance_index,
    timestep_index,
):
    cfg_index = lax.axis_index("cfg")
    seq_index = lax.axis_index("seq")
    seq_count = lax.axis_size("seq")
    dp_count = lax.axis_size("dp")
    tok_here = hidden.shape[2]
    length = tok_here * seq_count
    total_rows = 2 * dp_count * length
    ranks = 3 * ADAPTER_RANK
    input_features = hidden[0, 0]
    model_width = input_features.shape[1]
    half_cols = model_width // (2 * seq_count)

    guide_scale = 1.0 + 0.5 * guidance_index[:, 0].astype(jnp.float32)
    time_frac = (timestep_index[:, 0].astype(jnp.float32) + 0.5) / TSTEPS
    own_scale = lax.dynamic_index_in_dim(guide_scale, cfg_index, 0, keepdims=False)
    own_time = lax.dynamic_index_in_dim(time_frac, cfg_index, 0, keepdims=False)
    weighting = jnp.where(cfg_index == 0, guide_scale, 1.0 - guide_scale)
    rank_index = jnp.arange(1, ADAPTER_RANK + 1).astype(jnp.float32)
    feature_modulation = 1.0 + 0.5 * jnp.cos(
        math.pi * rank_index * own_time + 0.25 * rank_index * own_scale
    )
    modulation = jnp.tile(feature_modulation, 3)[None]

    teacher_heads, sent = scatter_teacher(
        (teacher_query[0, :, 0], teacher_key[0, :, 0], teacher_value[0, :, 0])
    )

    rank_projected = jnp.concatenate(
        [dot_f32(input_features, adapter_down_weight[member]) for member in range(3)], axis=1
    )
    rank_projected = (rank_projected * modulation).astype(jnp.bfloat16)
    rank_projected, *teacher_heads = lax.optimization_barrier((rank_projected, *teacher_heads))
    rank_all = gathered(rank_projected, "seq")
    rank_all = rank_all.reshape(length, ranks)

    split_view = input_features.reshape(tok_here, 2, seq_count, half_cols)
    split_view, rank_all = lax.optimization_barrier((split_view, rank_all))
    split_view = split_view.transpose(2, 0, 1, 3).reshape(seq_count, tok_here, 2 * half_cols)
    column_block = exchanged(split_view, "seq")
    column_block = column_block.reshape(length, 2 * half_cols)

    other = 1 - cfg_index
    other_weighted = teacher_attention(
        other, lax.dynamic_index_in_dim(weighting, other, 0, keepdims=False), teacher_heads
    )
    target_sent = lax.ppermute(other_weighted, "cfg", [(0, 1), (1, 0)])
    target_own = teacher_attention(
        cfg_index,
        lax.dynamic_index_in_dim(weighting, cfg_index, 0, keepdims=False),
        teacher_heads,
    )

    columns = target_own.shape[1]
    up_here = lax.dynamic_slice_in_dim(adapter_up_weight, seq_index * columns, columns, axis=2)
    student_local, up_partial, back_partial = student_step(
        cfg_index, total_rows, teacher_heads, sent, rank_all, up_here, target_own, target_sent
    )

    student_local, up_partial, back_partial, column_block = lax.optimization_barrier(
        (student_local, up_partial, back_partial, column_block)
    )
    groups = 2 * dp_count
    up_rows = ADAPTER_RANK // groups
    up_blocks = up_partial.reshape(3, groups, up_rows, columns).transpose(1, 0, 2, 3)
    student_tokens, grad_up, grad_rows = tail_exchange(
        back_partial, student_local, up_blocks, modulation
    )

    column_partial = lax.dot_general(
        column_block, grad_rows, TN, preferred_element_type=jnp.float32
    ).astype(jnp.bfloat16)
    down_rows = 2 * half_cols // groups
    down_parts = exchanged(column_partial.reshape(groups, down_rows, ranks), ("cfg", "dp"))
    grad_down = jnp.sum(down_parts.astype(jnp.float32), axis=0)
    grad_down = grad_down.reshape(down_rows, 3, ADAPTER_RANK).transpose(1, 0, 2)
    return (student_tokens[None, None], grad_down, grad_up)


def solution(mesh):
    placed = (
        P("cfg", None, "dp", "seq", None),
        P("cfg", None, "dp", "seq", None),
        P("cfg", None, "dp", "seq", None),
        P("cfg", "dp", "seq", None),
        P(),
        P(),
        P(None, "dp"),
        P(None, "dp"),
    )
    return jax.shard_map(
        body,
        mesh=mesh,
        in_specs=placed,
        out_specs=(
            P("cfg", "dp", "seq", None),
            P(None, ("cfg", "seq", "dp"), None),
            P(None, ("cfg", "dp"), "seq"),
        ),
        check_vma=False,
    )
```
